32 devices in a mesh: ep: 8 (over z, y), tp: 4 (over x, core).
Axes of the slice: x: 2, y: 2, z: 4, core: 2. Of those that a mesh axis runs over, the one named last changes fastest.
Arguments:
- tokens: bfloat16 [1024, 4096], P('ep'), may hold values from -6 to 6
- expert_ids: int32 [1024, 2], P('ep'), may hold values from 0 to 7, all different within a row; in each aligned block of 128 rows (0 to 127, 128 to 255, ...) at most 64 rows name the same one
- gate_logits: float32 [1024, 2], P('ep'), may hold values from -6 to 6
- w_gate: bfloat16 [8, 4096, 14336], P('ep', None, 'tp'), may hold values from -0.09375 to 0.09375
- w_up: bfloat16 [8, 4096, 14336], P('ep', None, 'tp'), may hold values from -0.09375 to 0.09375
- w_down: bfloat16 [8, 14336, 4096], P('ep', 'tp'), may hold values from -0.046875 to 0.046875
Outputs:
- output: bfloat16 [1024, 4096], P('ep', 'tp')
The draws below stay inside these ranges and needn't reach their ends.
Inputs may be any that keep to these rules, and one draw needn't show every extreme that they name: `expert_ids`: the 2 ids of a token differ. Among the 128 rows of one index of ep no expert is named more than 64 times, a bound that some block reaches.
All inputs are finite; a program needn't handle non-finite values.
Results may differ from the reference program's by a relative error of at most 0.014.
Values may be sent and summed in bfloat16 or wider, within the bound.
A program may use at most 192 MiB of HBM per device.

```python
import math
import jax
import jax.numpy as jnp
import numpy as np
from jax import lax

D = 4096
FF = 14336
EXPERTS = 8
TOP = 2
TOK_DEV = 128
CAP = 64
GROUP = 1
TOKENS = 1024
N_EP = 8
N_TP = 4


def levels(own_key, shape, pieces, smallest, largest):
    gain, own = 1.0, jax.random.fold_in(own_key, 6)
    for dim, parts in pieces:
        heights = jnp.exp(jax.random.uniform(jax.random.fold_in(own, dim), (parts,), jnp.float32, smallest / len(pieces), largest / len(pieces)))
        gain = gain * jnp.repeat(heights, shape[dim] // parts).reshape([-1 if axis == dim else 1 for axis in range(len(shape))])
    return gain


def routed_block(rng, own, number, rows, amount, top, bound, slope):
    ranking = jax.random.permutation(rng, amount)
    packed, usual = load_shares(amount, rows * top, bound, slope, True), load_shares(amount, rows * top, bound, slope, False)
    places = jnp.arange(amount)

    def named(tallies, rotation):
        used = int((tallies > 0).sum())
        fixed = max(1, used // 4)
        shifted = fixed + (places - fixed + rotation * (used - fixed)) % max(1, amount - fixed)
        return jnp.zeros((amount,), jnp.int32).at[ranking[jnp.where(places < fixed, places, shifted)]].set(jnp.asarray(tallies, jnp.int32))

    tallies = jnp.where(number % 4 == 0, named(packed, number // 4), named(usual, number - number // 4 - 1))
    mixed = jax.random.permutation(jax.random.fold_in(own, 3), amount)
    giver, receiver = mixed[0:amount // 2 * 2:2], mixed[1:amount // 2 * 2:2]
    slack = jnp.minimum(tallies[giver] - 1, bound - tallies[receiver]) // 2
    slack = jnp.where((giver == ranking[0]) | (receiver == ranking[0]) | (tallies[receiver] == 0), 0, jnp.maximum(slack, 0))
    shifted = jax.random.randint(jax.random.fold_in(own, 4), (amount // 2,), 0, 1 << 20) % (slack + 1)
    tallies = tallies.at[giver].add(-shifted).at[receiver].add(shifted)
    members = jnp.searchsorted(jnp.cumsum(tallies), jnp.arange(rows * top), side="right").astype(jnp.int32)
    grid = members.reshape(top, rows).T
    grid = grid[jax.random.permutation(jax.random.fold_in(own, 1), rows)]
    rotation = jax.random.randint(jax.random.fold_in(own, 2), (rows, 1), 0, top)
    return jnp.take_along_axis(grid, (jnp.arange(top)[None, :] + rotation) % top, axis=1)


def load_shares(number_of, total, bound, skew, full):
    weights = [(1 << 20) // math.isqrt(standing ** skew) + 1 for standing in range(1, number_of + 1)]
    largest = bound if full else min(bound, max(-(-total // number_of), total * weights[0] // sum(weights)))
    least = 1 if total - largest >= number_of - 1 else 0
    given, surplus = [largest] + [least] * (number_of - 1), total - largest - least * (number_of - 1)
    while surplus > 0:
        candidates = [i for i in range(1, number_of) if given[i] < largest] or [i for i in range(1, number_of) if given[i] < bound]
        mass, left = sum([weights[i] for i in candidates]), surplus
        for i in candidates:
            more = min(bound - given[i], max(1, left * weights[i] // mass), surplus)
            given[i] = given[i] + more
            surplus = surplus - more
    return np.array(given)


def centred(own_key, extent, spread, most, cuts=(), kind=jnp.bfloat16):
    entries = spread * jax.random.normal(own_key, extent, jnp.float32)
    if cuts:
        entries = entries * levels(own_key, extent, cuts, -0.22, 0.18)
    return jnp.clip(entries, -most, most).astype(kind)


def setup_inputs(seed: int = 0) -> dict:
    streams_of = jax.random.split(jax.random.key(seed), 7)
    tokens = centred(streams_of[0], (TOKENS, D), 1.0, 6.0, ((0, 8),))
    expert_ids_keys = jax.random.split(jax.random.fold_in(streams_of[1], 1), TOKENS // TOK_DEV)
    expert_ids_turns = jax.random.permutation(jax.random.fold_in(streams_of[1], 3), TOKENS // TOK_DEV)
    expert_ids = jax.vmap(lambda own, number: routed_block(jax.random.fold_in(streams_of[1], 2), own, number, TOK_DEV, EXPERTS, TOP, CAP, 1))(expert_ids_keys, expert_ids_turns).reshape((TOKENS, TOP))
    gate_logits = centred(streams_of[2], (TOKENS, TOP), 1.5, 6.0, ((0, 8),), jnp.float32)
    w_gate = centred(streams_of[3], (N_EP, D, FF // GROUP), D ** -0.5, 0.09375, ((0, 8), (2, 4)))
    w_up = centred(streams_of[4], (N_EP, D, FF // GROUP), D ** -0.5, 0.09375, ((0, 8), (2, 4)))
    w_down = centred(streams_of[5], (N_EP, FF // GROUP, D), FF ** -0.5, 0.046875, ((0, 8), (1, 4)))
    return dict(tokens=tokens, expert_ids=expert_ids, gate_logits=gate_logits, w_gate=w_gate, w_up=w_up, w_down=w_down)


def reference(tokens, expert_ids, gate_logits, w_gate, w_up, w_down):
    first = 1.0 / (1.0 + jnp.exp(gate_logits[:, 1] - gate_logits[:, 0]))
    second = 1.0 / (1.0 + jnp.exp(gate_logits[:, 0] - gate_logits[:, 1]))
    gate_weights = jnp.stack([first, second], axis=1).astype(jnp.float32)
    blocked = expert_ids.reshape(N_EP, TOK_DEV * TOP)
    onehot = (blocked[:, :, None] == jnp.arange(EXPERTS, dtype=jnp.int32)[None, None, :]).astype(jnp.int32)
    before = jnp.cumsum(onehot, axis=1) - onehot
    slot = jnp.sum(before * onehot, axis=2).astype(jnp.int32)
    source = jnp.arange(N_EP, dtype=jnp.int32)[:, None]
    dest = (source * CAP + slot).reshape(-1).astype(jnp.int32)
    flat_ids = expert_ids.reshape(-1).astype(jnp.int32)
    repeated = jnp.repeat(tokens, TOP, axis=0)
    buffers = jnp.zeros((EXPERTS, N_EP * CAP, D), jnp.bfloat16).at[flat_ids, dest].set(repeated)
    gate_slabs = w_gate.reshape(EXPERTS, GROUP, D, FF // GROUP)
    up_slabs = w_up.reshape(EXPERTS, GROUP, D, FF // GROUP)
    down_full = w_down.reshape(EXPERTS, FF, D)
    split = GROUP * N_TP
    width = FF // split

    def expert(items):
        rows, gslab, uslab, down = items
        gmat = jnp.concatenate([gslab[g] for g in range(GROUP)], axis=1)
        umat = jnp.concatenate([uslab[g] for g in range(GROUP)], axis=1)
        gate = jnp.dot(rows, gmat, preferred_element_type=jnp.float32)
        upper = jnp.dot(rows, umat, preferred_element_type=jnp.float32)
        hidden = (jax.nn.silu(gate) * upper).astype(jnp.bfloat16)

        def add_group(j, total):
            start = (j * width).astype(jnp.int32)
            piece = lax.dynamic_slice_in_dim(hidden, start, width, 1)
            wpiece = lax.dynamic_slice_in_dim(down, start, width, 0)
            part = jnp.dot(piece, wpiece, preferred_element_type=jnp.float32).astype(jnp.bfloat16)
            part = lax.optimization_barrier(part)
            return total + part.astype(jnp.float32)

        return lax.fori_loop(0, split, add_group, jnp.zeros((N_EP * CAP, D), jnp.float32))

    results = lax.map(expert, (buffers, gate_slabs, up_slabs, down_full))
    picked = results[flat_ids, dest].reshape(TOKENS, TOP, D)
    combined = jnp.sum(gate_weights[:, :, None] * picked, axis=1)
    return combined.astype(jnp.bfloat16)
```

```python
import functools

import jax
import jax.numpy as jnp
from jax import lax
from jax.experimental import pallas as pl
from jax.experimental.pallas import tpu as pltpu
from jax.sharding import PartitionSpec as P

EXPERTS = 8
TOP = 2
CORES = 2
MESH = pl.DeviceIdType.MESH


def tile_of(extent, most):
    width = most
    while extent % width:
        width -= 128
    return width


def layer(
    sources, planes, cap, tn, td,
    packed, wg, wu, wd, ret,
    xbuf, gacc, uacc, hid, wbuf, dbuf, psend, precv, own, xsend, xrecv, esend,
    wsem, dsem, lsem, es, er, xs, xr, cs, cr, fs, fr, ps, pr, ys, yr, zs, zr,
):
    me = lax.axis_index("ep")
    tp = lax.axis_index("tp")
    core = lax.rem(tp, CORES)
    plane = tp // CORES
    other = plane * CORES + lax.rem(core + 1, CORES)
    teams = planes * CORES
    share = packed.shape[2]
    hidden = hid.shape[1]
    ntiles = hidden // tn
    dtiles = share // td
    total = teams * ntiles

    def peer(dx):
        return lax.rem(plane + dx, planes) * CORES + core

    def quarter(qi):
        return lax.rem(plane + planes - qi // CORES, planes) * CORES + lax.rem(core + qi % CORES, CORES)

    def weights(i, which, src):
        rows = pl.ds(pl.multiple_of(quarter(i // ntiles) * share, share), share)
        cols = pl.ds(pl.multiple_of((i % ntiles) * tn, tn), tn)
        return pltpu.make_async_copy(src.at[rows, cols], wbuf.at[i % 3, which], wsem.at[i % 3, which])

    def fetch(i):
        weights(i, 0, wg).start()
        weights(i, 1, wu).start()

    def chunk(ci):
        dx = lax.rem(ci // CORES + 1, planes)
        return lax.rem(plane + dx, planes) * CORES + lax.rem(core + 1 + ci % CORES, CORES)

    def down(i):
        cols = pl.ds(pl.multiple_of(chunk(i // dtiles) * share + (i % dtiles) * td, td), td)
        return pltpu.make_async_copy(wd.at[:, cols], dbuf.at[i % 3], dsem.at[i % 3])

    fetch(0)
    fetch(1)
    for i in range(2):
        down(i).start()

    barrier = pltpu.get_barrier_semaphore()
    for k in range(1, sources):
        pl.semaphore_signal(barrier, inc=1, device_id={"ep": lax.rem(me + k, sources), "tp": tp}, device_id_type=MESH)
    for dx in range(1, planes):
        pl.semaphore_signal(barrier, inc=1, device_id={"ep": me, "tp": peer(dx)}, device_id_type=MESH)
    pl.semaphore_signal(barrier, inc=1, device_id={"ep": me, "tp": other}, device_id_type=MESH)
    pl.semaphore_wait(barrier, sources - 1 + planes - 1 + 1)

    def rows_of(s):
        return pl.ds(pl.multiple_of(s * cap, cap), cap)

    ep_copies = [None]
    for k in range(1, sources):
        to = lax.rem(me + k, sources)
        copy = pltpu.make_async_remote_copy(
            src_ref=packed.at[to], dst_ref=xbuf.at[tp, rows_of(me)],
            send_sem=es.at[k], recv_sem=er.at[k],
            device_id={"ep": to, "tp": tp}, device_id_type=MESH)
        copy.start()
        ep_copies.append(copy)
    local = pltpu.make_async_copy(packed.at[me], xbuf.at[tp, rows_of(me)], lsem.at[0])
    local.start()
    local.wait()
    x_copies, c_copies = {}, []
    for k in range(sources):
        s = lax.rem(me - k + sources, sources)
        if k:
            ep_copies[k].wait_recv()
        for dx in range(1, planes):
            copy = pltpu.make_async_remote_copy(
                src_ref=xbuf.at[tp, rows_of(s)], dst_ref=xbuf.at[tp, rows_of(s)],
                send_sem=xs.at[dx, k], recv_sem=xr.at[dx, k],
                device_id={"ep": me, "tp": peer(dx)}, device_id_type=MESH)
            copy.start()
            x_copies[dx, k] = copy
        copy = pltpu.make_async_remote_copy(
            src_ref=xbuf.at[tp, rows_of(s)], dst_ref=xbuf.at[tp, rows_of(s)],
            send_sem=cs.at[k], recv_sem=cr.at[k],
            device_id={"ep": me, "tp": other}, device_id_type=MESH)
        copy.start()
        c_copies.append(copy)

    f_copies = {}
    for qi in range(teams):
        dx = qi // CORES
        q = quarter(qi)
        if qi == 1:
            for copy in c_copies:
                copy.wait_recv()
        elif qi > 1 and qi % CORES == 0:
            for k in range(sources):
                x_copies[dx, k].wait_recv()
            copy = pltpu.make_async_remote_copy(
                src_ref=xbuf.at[q], dst_ref=xbuf.at[q],
                send_sem=fs.at[dx], recv_sem=fr.at[dx],
                device_id={"ep": me, "tp": other}, device_id_type=MESH)
            copy.start()
            f_copies[dx] = copy
        elif qi > 1:
            f_copies[dx].wait_recv()

        def step(n, carry, qi=qi, q=q):
            i = qi * ntiles + n

            @pl.when(i + 2 < total)
            def _():
                fetch(i + 2)

            weights(i, 0, wg).wait()
            weights(i, 1, wu).wait()
            cols = pl.ds(pl.multiple_of(n * tn, tn), tn)
            gate = jnp.dot(xbuf[q], wbuf[i % 3, 0], preferred_element_type=jnp.float32)
            upper = jnp.dot(xbuf[q], wbuf[i % 3, 1], preferred_element_type=jnp.float32)
            if qi:
                gate = gate + gacc[:, cols]
                upper = upper + uacc[:, cols]
            if qi < teams - 1:
                gacc[:, cols] = gate
                uacc[:, cols] = upper
            else:
                hid[:, cols] = (gate / (1.0 + jnp.exp(-gate)) * upper).astype(jnp.bfloat16)
            return carry

        lax.fori_loop(0, ntiles, step, 0)

    dtotal = teams * dtiles
    p_copies, y_copies = {}, {}
    for ci in range(teams):
        dx = (ci // CORES + 1) % planes
        mine = ci % CORES == 1

        def dstep(n, carry, ci=ci, dx=dx, mine=mine):
            i = ci * dtiles + n

            @pl.when(i + 2 < dtotal)
            def _():
                down(i + 2).start()

            down(i).wait()
            cols = pl.ds(pl.multiple_of(n * td, td), td)
            part = jnp.dot(hid[...], dbuf[i % 3], preferred_element_type=jnp.float32)
            if mine:
                own[:, cols] = part
            else:
                psend[dx, :, cols] = part.astype(jnp.bfloat16)
            return carry

        lax.fori_loop(0, dtiles, dstep, 0)
        if not mine:
            copy = pltpu.make_async_remote_copy(
                src_ref=psend.at[dx], dst_ref=precv.at[dx],
                send_sem=ps.at[dx], recv_sem=pr.at[dx],
                device_id={"ep": me, "tp": other}, device_id_type=MESH)
            copy.start()
            p_copies[dx] = copy
        elif dx:
            p_copies[dx].wait_recv()
            for k in range(sources):
                s = lax.rem(me + k + 1, sources)
                rows = rows_of(s)
                xsend[dx - 1, rows] = (own[rows] + precv[dx, rows].astype(jnp.float32)).astype(jnp.bfloat16)
                copy = pltpu.make_async_remote_copy(
                    src_ref=xsend.at[dx - 1, rows], dst_ref=xrecv.at[dx - 1, rows],
                    send_sem=ys.at[dx, k], recv_sem=yr.at[dx, k],
                    device_id={"ep": me, "tp": peer(dx)}, device_id_type=MESH)
                copy.start()
                y_copies[dx, k] = copy
    p_copies[0].wait_recv()
    z_copies = []
    for k in range(sources):
        s = lax.rem(me + k + 1, sources)
        rows = rows_of(s)
        value = own[rows] + precv[0, rows].astype(jnp.float32)
        for dx in range(1, planes):
            y_copies[dx, k].wait_recv()
            value = value + xrecv[dx - 1, rows].astype(jnp.float32)
        if k == sources - 1:
            ret[me] = value.astype(jnp.bfloat16)
        else:
            esend[k] = value.astype(jnp.bfloat16)
            copy = pltpu.make_async_remote_copy(
                src_ref=esend.at[k], dst_ref=ret.at[me],
                send_sem=zs.at[k], recv_sem=zr.at[k],
                device_id={"ep": s, "tp": tp}, device_id_type=MESH)
            copy.start()
            z_copies.append(copy)
    for copy in z_copies:
        copy.wait_recv()
    for copy in ep_copies[1:] + list(x_copies.values()) + c_copies + list(f_copies.values()):
        copy.wait_send()
    for copy in list(p_copies.values()) + list(y_copies.values()) + z_copies:
        copy.wait_send()


def shards(tokens, expert_ids, gate_logits, w_gate, w_up, w_down):
    tok_count, width = tokens.shape
    ep_count = lax.axis_size("ep")
    tp_count = lax.axis_size("tp")
    group = ep_count // EXPERTS
    cap = tok_count // 2
    share = width // tp_count
    planes = tp_count // CORES
    hidden = w_gate.shape[2]
    first = 1.0 / (1.0 + jnp.exp(gate_logits[:, 1] - gate_logits[:, 0]))
    second = 1.0 / (1.0 + jnp.exp(gate_logits[:, 0] - gate_logits[:, 1]))
    experts = jnp.arange(EXPERTS, dtype=jnp.int32)[None, :]
    hit0 = expert_ids[:, 0:1] == experts
    hit1 = expert_ids[:, 1:2] == experts
    row = lax.broadcasted_iota(jnp.int32, (tok_count, tok_count), 0)
    col = lax.broadcasted_iota(jnp.int32, (tok_count, tok_count), 1)
    earlier = jnp.dot(
        (col < row).astype(jnp.bfloat16), (hit0 | hit1).astype(jnp.bfloat16),
        preferred_element_type=jnp.float32).astype(jnp.int32)
    dest0 = jnp.sum(jnp.where(hit0, earlier + experts * cap, 0), axis=1)
    dest1 = jnp.sum(jnp.where(hit1, earlier + experts * cap, 0), axis=1)
    places = jnp.arange(EXPERTS * cap, dtype=jnp.int32)
    pick = ((places[:, None] == dest0[None, :]) | (places[:, None] == dest1[None, :])).astype(jnp.bfloat16)
    quarter = lax.dynamic_slice_in_dim(tokens, lax.axis_index("tp") * share, share, 1)
    packed = jnp.dot(pick, quarter, preferred_element_type=jnp.float32).astype(jnp.bfloat16)
    packed = jnp.repeat(packed.reshape(EXPERTS, cap, share), group, axis=0)

    tn = tile_of(hidden, 512)
    td = tile_of(share, 256)
    rows = ep_count * cap
    vmem = pl.BlockSpec(memory_space=pltpu.VMEM)
    hbm = pl.BlockSpec(memory_space=pl.ANY)
    dma = pltpu.SemaphoreType.DMA
    bf16, f32 = jnp.bfloat16, jnp.float32
    ret = pl.pallas_call(
        functools.partial(layer, ep_count, planes, cap, tn, td),
        out_shape=jax.ShapeDtypeStruct((ep_count, cap, share), bf16),
        in_specs=[vmem, hbm, hbm, hbm],
        out_specs=vmem,
        scratch_shapes=[
            pltpu.VMEM((tp_count, rows, share), bf16),
            pltpu.VMEM((rows, hidden), f32),
            pltpu.VMEM((rows, hidden), f32),
            pltpu.VMEM((rows, hidden), bf16),
            pltpu.VMEM((3, 2, share, tn), bf16),
            pltpu.VMEM((3, hidden, td), bf16),
            pltpu.VMEM((planes, rows, share), bf16),
            pltpu.VMEM((planes, rows, share), bf16),
            pltpu.VMEM((rows, share), f32),
            pltpu.VMEM((planes - 1, rows, share), bf16),
            pltpu.VMEM((planes - 1, rows, share), bf16),
            pltpu.VMEM((ep_count, cap, share), bf16),
            dma((3, 2)),
            dma((3,)),
            dma((1,)),
            dma((ep_count,)), dma((ep_count,)),
            dma((planes, ep_count)), dma((planes, ep_count)),
            dma((ep_count,)), dma((ep_count,)),
            dma((planes,)), dma((planes,)),
            dma((planes,)), dma((planes,)),
            dma((planes, ep_count)), dma((planes, ep_count)),
            dma((ep_count,)), dma((ep_count,)),
        ],
        compiler_params=pltpu.CompilerParams(
            collective_id=0, has_side_effects=True, vmem_limit_bytes=60 * 1024 * 1024),
        name="expert_layer",
    )(packed, w_gate[0], w_up[0], w_down[0])

    results = ret.reshape(EXPERTS * group * cap, share)
    home = jnp.arange(EXPERTS * group * cap, dtype=jnp.int32)[None, :]
    slot_at = (home // (group * cap)) * cap + home % cap
    out0 = jnp.dot((slot_at == dest0[:, None]).astype(bf16), results, preferred_element_type=f32)
    out1 = jnp.dot((slot_at == dest1[:, None]).astype(bf16), results, preferred_element_type=f32)
    return (first[:, None] * out0 + second[:, None] * out1).astype(bf16)


def solution(mesh):
    placed = (
        P("ep", None),
        P("ep", None),
        P("ep", None),
        P("ep", None, "tp"),
        P("ep", None, "tp"),
        P("ep", "tp", None),
    )
    return jax.shard_map(
        shards, mesh=mesh, in_specs=placed, out_specs=P("ep", "tp"), check_vma=False
    )
```
